32 devices in a mesh: vocab: 16 (over z, y, x), batch: 2 (over core).
Axes of the slice: x: 2, y: 2, z: 4, core: 2. Of those that a mesh axis runs over, the one named last changes fastest.
Arguments:
- hidden: bfloat16 [2048, 7168], P(('batch', 'vocab')), parts along dimension 0, may hold values from -1000 to 1000
- norm_gain: bfloat16 [7168], replicated, may hold values from 1.5 to 5
- lm_head: bfloat16 [7168, 16384], P(None, 'vocab'), may hold values from -2 to 2
- draft_logits: bfloat16 [2048, 16384], P('batch', 'vocab'), parts along dimension 0, may hold values from -480 to 480
- draft_tokens: int32 [2048], P('batch'), parts along dimension 0, may hold values from 0 to 16383
- tree_parents: int32 [2048], P('batch'), parts along dimension 0, may hold values from 0 to 62, as said below
- node_depths: int32 [2048], P('batch'), parts along dimension 0, may hold values from 0 to 8, as said below
- uniforms: float32 [2048], P('batch'), parts along dimension 0, may hold values from 0 to 1
Outputs:
- target_lse: float32 [2048], P('batch'), parts along dimension 0
- token_logprob: float32 [2048], P('batch'), parts along dimension 0
- residual_mass: float32 [2048], P('batch'), parts along dimension 0
- accept_margin: float32 [2048], P('batch'), parts along dimension 0
- path_margin: float32 [2048], P('batch'), parts along dimension 0
The draws below stay inside these ranges and needn't reach their ends.
There are 2 independent parts, one for each index of `batch`. The reference program is written for one: setup_inputs(seed, part) draws one part's arguments, and reference() takes and returns one part's arrays. A program takes and returns all parts, laid end to end along the dimension named above; an argument that names none is the same for every part. Nothing has to cross between parts.
Inputs may be any that keep to these rules, and one draw needn't show every extreme that they name: `tree_parents`: rows come in 16 requests of 64 consecutive rows, the first of each being the root. A node's entry is the position of its parent within the request, smaller than its own position; the root's entry is 0. `node_depths`: A node's depth is its parent's depth plus one, the root's is 0; in every request some node has depth 8.
All inputs are finite; a program needn't handle non-finite values.
Results may differ from the reference program's by a relative error of at most 0.0049.
Values may be sent and summed in bfloat16 or wider, within the bound.
A program may use at most 128 MiB of HBM per device.

```python
import math
import jax
import jax.numpy as jnp
import numpy as np
from jax import lax

D = 7168
VOCAB = 16384
NODES = 64
DEPTH_MAX = 8
REQ = 16
ROWS = 1024


def draw_hidden(key, part):
    gaussian = jax.random.normal(jax.random.fold_in(key, 11), (ROWS, D), jnp.float32)
    return jnp.clip(gaussian, -6.0, 6.0).astype(jnp.bfloat16)


def draw_lm_head(key, part):
    gaussian = jax.random.normal(jax.random.fold_in(key, 21), (D, VOCAB), jnp.float32)
    columns = jnp.arange(VOCAB, dtype=jnp.int32)
    position = columns.astype(jnp.float32) / VOCAB
    weights = gaussian * (1.0 + 0.1 * position) / math.sqrt(D)
    return jnp.clip(weights, -2.0, 2.0).astype(jnp.bfloat16)


def draw_draft_logits(key, part):
    gaussian = jax.random.normal(jax.random.fold_in(key, 31), (ROWS, VOCAB), jnp.float32)
    columns = jnp.arange(VOCAB, dtype=jnp.int32)
    position = columns.astype(jnp.float32) / VOCAB
    return jnp.clip(3.0 * gaussian * (1.0 + 0.1 * position), -24.0, 24.0).astype(jnp.bfloat16)


def build_tree(key):
    jitter = jax.random.randint(jax.random.fold_in(key, 41), (REQ, NODES, NODES), 0, 4096)
    positions = jnp.arange(NODES, dtype=jnp.int32)

    def grow_tree(jitter_request):

        def add_node(carry, node_index):
            depths, deepest = carry
            eligible = (positions < node_index) & (depths < DEPTH_MAX)
            forced = NODES - node_index <= DEPTH_MAX - deepest
            ranked = jnp.where(forced, depths * 65536 + positions, (jitter_request[node_index] + 1024 * depths) * 64 + positions)
            ranked = jnp.where(eligible, ranked, -1)
            chosen_parent = jnp.argmax(ranked).astype(jnp.int32)
            new_depth = depths[chosen_parent] + 1
            depths = depths.at[node_index].set(new_depth)
            return ((depths, jnp.maximum(deepest, new_depth)), (chosen_parent, new_depth))
        initial = (jnp.zeros((NODES,), jnp.int32), jnp.int32(0))
        _, (parents, depths) = lax.scan(add_node, initial, jnp.arange(1, NODES, dtype=jnp.int32))
        anchor = jnp.zeros((1,), jnp.int32)
        return (jnp.concatenate([anchor, parents]), jnp.concatenate([anchor, depths]))
    parents, depths = jax.vmap(grow_tree)(jitter)
    return (parents.reshape(ROWS).astype(jnp.int32), depths.reshape(ROWS).astype(jnp.int32))


def draw_tree_parents(key, part):
    return build_tree(key)[0]


def draw_node_depths(key, part):
    return build_tree(key)[1]


def set_ends(values, rng, low, largest):
    longest = values.shape.index(max(values.shape))
    spots = []
    for shift in (0, 1):
        where = [jax.random.randint(jax.random.fold_in(rng, axis), (), 0, length) for axis, length in enumerate(values.shape)]
        where[longest] = (where[longest] + shift) % values.shape[longest]
        spots.append(tuple(where))
    return values.at[spots[0]].set(low).at[spots[1]].set(largest)


def cumulative_ranks(amount, lean):
    loads = [(1 << 20) // math.isqrt(rank ** lean) + 1 for rank in range(1, amount + 1)]
    width = 1 + sum(loads) // (1 << 30)
    return np.cumsum(np.array([max(1, weight // width) for weight in loads]))


def ranked_ids(rng, dims, number_of, slope):
    grid = cumulative_ranks(number_of, slope)
    lot = jax.random.randint(jax.random.fold_in(rng, 1), dims, 0, int(grid[number_of - 1]))
    standing = jnp.searchsorted(jnp.asarray(grid, jnp.int32), lot, side="right")
    return jax.random.permutation(jax.random.fold_in(rng, 2), number_of)[standing].astype(jnp.int32)


def setup_inputs(seed: int = 0, part: int = 0) -> dict:
    key_list = jax.random.split(jax.random.key(seed), 9)
    part_splits = jax.random.split(jax.random.fold_in(key_list[8], part), 9)
    return {
        "hidden": draw_hidden(jax.random.fold_in(jax.random.fold_in(key_list[8], part), 71), part),
        "norm_gain": jnp.clip(jnp.exp(jax.random.uniform(key_list[1], (D,), jnp.float32, math.log(1.5), math.log(5.0))), 1.5, 5.0).astype(jnp.bfloat16),
        "lm_head": draw_lm_head(jax.random.fold_in(key_list[8], 71), part),
        "draft_logits": draw_draft_logits(jax.random.fold_in(jax.random.fold_in(key_list[8], part), 71), part),
        "draft_tokens": set_ends(ranked_ids(part_splits[4], (ROWS,), VOCAB, 2), jax.random.fold_in(part_splits[4], 3), 0, VOCAB - 1).astype(jnp.int32),
        "tree_parents": draw_tree_parents(jax.random.fold_in(jax.random.fold_in(key_list[8], part), 71), part),
        "node_depths": draw_node_depths(jax.random.fold_in(jax.random.fold_in(key_list[8], part), 71), part),
        "uniforms": jnp.clip(jax.random.uniform(part_splits[7], (ROWS,), jnp.float32, 0.0, 1.0), 0.0, 1.0),
    }


epsilon = 1e-06

def normalize(hidden_rows, gain_vector):
    values = hidden_rows.astype(jnp.float32)
    mean_square = lax.optimization_barrier(jnp.mean(values * values, axis=1, keepdims=True))
    scaled = values * lax.rsqrt(mean_square + epsilon) * gain_vector.astype(jnp.float32)
    return scaled.astype(jnp.bfloat16)

def log_total(scores):
    row_max = lax.optimization_barrier(jnp.max(scores, axis=1))
    return row_max + jnp.log(lax.optimization_barrier(jnp.sum(jnp.exp(scores - row_max[:, None]), axis=1)))

def reference(hidden, norm_gain, lm_head, draft_logits, draft_tokens, tree_parents, node_depths, uniforms):
    normed = normalize(hidden, norm_gain)
    logits = jnp.dot(normed, lm_head, preferred_element_type=jnp.float32)
    draft_values = draft_logits.astype(jnp.float32)
    target_lse = log_total(logits)
    draft_lse = log_total(draft_values)
    positions = jnp.arange(ROWS, dtype=jnp.int32)
    parent_row = (positions - positions % NODES + tree_parents).astype(jnp.int32)
    token_logprob = logits[parent_row, draft_tokens] - target_lse[parent_row]
    draft_logprob = draft_values[parent_row, draft_tokens] - draft_lse[parent_row]
    accept_margin = jnp.exp(jnp.minimum(token_logprob - draft_logprob, 0.0)) - uniforms
    target_prob = jnp.exp(logits - target_lse[:, None])
    draft_prob = jnp.exp(draft_values - draft_lse[:, None])
    residual_mass = lax.optimization_barrier(jnp.sum(jnp.maximum(target_prob - draft_prob, 0.0), axis=1))
    path_margin = jnp.ones((ROWS,), jnp.float32)
    for level_now in range(1, DEPTH_MAX + 1):
        path_margin = jnp.where(node_depths == level_now, jnp.minimum(accept_margin, path_margin[parent_row]), path_margin)
    return (target_lse, token_logprob, residual_mass, accept_margin, path_margin)
```

```python
import functools

import jax
import jax.numpy as jnp
from jax import lax
from jax.experimental import pallas as pl
from jax.experimental.pallas import tpu as pltpu
from jax.sharding import PartitionSpec as P

NODES = 64
DEPTH_MAX = 8
MESH = pl.DeviceIdType.MESH
CHUNK_ROWS = 256
COLUMN_TILE = 256


epsilon = 1e-06
highest = lax.Precision.HIGHEST


def normalize(hidden_rows, gain_vector):
    values = hidden_rows.astype(jnp.float32)
    mean_square = jnp.mean(values * values, axis=1, keepdims=True)
    scaled = values * lax.rsqrt(mean_square + epsilon) * gain_vector.astype(jnp.float32)
    return scaled.astype(jnp.bfloat16)


def place_of(device, cycle, n):
    if n != 16:
        return device
    z, y, x = device // 4, (device // 2) % 2, device % 2
    corner = 2 * y + (x + y) % 2
    step = (corner + z) % 4
    return 4 * (z if cycle == 0 else corner) + step


def device_at(place, cycle, n):
    if n != 16:
        return place
    major = place // 4
    minor = (place % 4 + 4 - major) % 4
    z, corner = (major, minor) if cycle == 0 else (minor, major)
    y = corner // 2
    x = (corner + y) % 2
    return 4 * z + 2 * y + x


def gather_dot_kernel(
    n, parts, own_ref, head_ref, out_ref, held, head, own_sem, head_sem, send_sem, recv_sem
):
    streams, rows, width = own_ref.shape
    group = max(1, min(n, CHUNK_ROWS // rows))
    chunks = n // group
    columns = out_ref.shape[2]
    me = lax.axis_index("vocab")
    places = [place_of(me, cycle, n) for cycle in range(2)]

    def stream_kind(q):
        lane = q // parts
        return lane // 2, lane % 2

    def partner(q, steps):
        cycle, backward = stream_kind(q)
        hop = (n - steps) if backward else steps
        return device_at(lax.rem(places[cycle] + hop, n), cycle, n)

    own_copy = pltpu.make_async_copy(own_ref, held.at[0], own_sem)
    own_copy.start()
    head_copy = pltpu.make_async_copy(head_ref, head, head_sem)
    head_copy.start()

    ways = [partner(q, 1) for q in range(0, streams, parts)]
    barrier = pltpu.get_barrier_semaphore()
    for target in ways:
        pl.semaphore_signal(barrier, inc=1, device_id={"vocab": target}, device_id_type=MESH)
    pl.semaphore_wait(barrier, len(ways))

    def copy_of(q, step):
        return pltpu.make_async_remote_copy(
            src_ref=held.at[step, q],
            dst_ref=held.at[step + 1, q],
            send_sem=send_sem.at[step, q],
            recv_sem=recv_sem.at[step, q],
            device_id={"vocab": ways[q // parts]},
            device_id_type=MESH,
        )

    def multiply(chunk, q):
        first = chunk * group

        def tile(index, _):
            at = pl.multiple_of(index * COLUMN_TILE, COLUMN_TILE)
            block = jnp.concatenate([held[first + g, q] for g in range(group)], axis=0)
            part = jnp.dot(
                block, head[q, :, pl.ds(at, COLUMN_TILE)], preferred_element_type=jnp.float32
            )
            for g in range(group):
                cycle, backward = stream_kind(q)
                slot = first + g
                place = places[cycle] + slot if backward else places[cycle] + n - slot
                owner = device_at(lax.rem(place, n), cycle, n)
                piece = part[g * rows : (g + 1) * rows]
                out_ref[owner, :, pl.ds(at, COLUMN_TILE)] += piece
            return 0

        lax.fori_loop(0, columns // COLUMN_TILE, tile, 0)

    own_copy.wait()
    for q in range(streams):
        copy_of(q, 0).start()
    head_copy.wait()
    out_ref[...] = jnp.zeros_like(out_ref)

    return me, group, chunks, copy_of, multiply


def gather_dot_body(n, parts, *refs):
    streams = refs[0].shape[0]
    _, group, chunks, copy_of, multiply = gather_dot_kernel(n, parts, *refs)
    per_step = streams // group if group <= streams else 1
    spread = streams // per_step

    def run(chunk, turn):
        for k in range(per_step):
            q = turn * per_step + k
            if q < streams:
                multiply(chunk, q)

    def move(step):
        for q in range(streams):
            copy_of(q, step - 1).wait_recv()
            copy_of(q, step).start()

    def chunk_loop(chunk, _):
        for g in range(group):
            move(chunk * group + g)
            if g < spread:
                run(chunk - 1, g)
        return 0

    for step in range(1, group):
        move(step)
    lax.fori_loop(1, chunks - 1, chunk_loop, 0)
    for g in range(group):
        step = (chunks - 1) * group + g
        if step < n - 1:
            move(step)
        else:
            for q in range(streams):
                copy_of(q, step - 1).wait_recv()
        if g < spread:
            run(chunks - 2, g)
    for q in range(streams):
        multiply(chunks - 1, q)

    def drain(step, _):
        for q in range(streams):
            copy_of(q, step).wait_send()
        return 0

    lax.fori_loop(0, n - 1, drain, 0)


def gather_dot(normed, lm_head, n):
    rows, depth = normed.shape
    parts = 2 if n <= 16 else 1
    streams = 4 * parts
    width = depth // streams
    columns = lm_head.shape[1]
    own = normed.reshape(rows, streams, width).transpose(1, 0, 2)
    out = pl.pallas_call(
        functools.partial(gather_dot_body, n, parts),
        out_shape=jax.ShapeDtypeStruct((n, rows, columns), jnp.float32),
        in_specs=[pl.BlockSpec(memory_space=pl.ANY)] * 2,
        out_specs=pl.BlockSpec(memory_space=pltpu.VMEM),
        scratch_shapes=[
            pltpu.VMEM((n, streams, rows, width), jnp.bfloat16),
            pltpu.VMEM((streams, width, columns), jnp.bfloat16),
            pltpu.SemaphoreType.DMA,
            pltpu.SemaphoreType.DMA,
            pltpu.SemaphoreType.DMA((n - 1, streams)),
            pltpu.SemaphoreType.DMA((n - 1, streams)),
        ],
        compiler_params=pltpu.CompilerParams(
            collective_id=0, has_side_effects=True, vmem_limit_bytes=56 * 1024 * 1024
        ),
        name="gather_dot",
    )(own, lm_head.reshape(streams, width, columns))
    return out.reshape(n * rows, columns)


def exchange_kernel(n, x_ref, out_ref, own_sem, send_sem, recv_sem):
    me = lax.axis_index("vocab")
    barrier = pltpu.get_barrier_semaphore()

    def copy_to(d):
        return pltpu.make_async_remote_copy(
            src_ref=x_ref,
            dst_ref=out_ref.at[me],
            send_sem=send_sem.at[d],
            recv_sem=recv_sem.at[d],
            device_id={"vocab": lax.rem(me + d, n)},
            device_id_type=MESH,
        )

    def copy_from(d):
        return pltpu.make_async_remote_copy(
            src_ref=x_ref,
            dst_ref=out_ref.at[lax.rem(me + n - d, n)],
            send_sem=send_sem.at[d],
            recv_sem=recv_sem.at[d],
            device_id={"vocab": lax.rem(me + d, n)},
            device_id_type=MESH,
        )

    def greet(d, _):
        pl.semaphore_signal(
            barrier, inc=1, device_id={"vocab": lax.rem(me + d, n)}, device_id_type=MESH
        )
        return 0

    def send(d, _):
        copy_to(d).start()
        return 0

    def finish(d, _):
        copy_from(d).wait_recv()
        copy_to(d).wait_send()
        return 0

    own_copy = pltpu.make_async_copy(x_ref, out_ref.at[me], own_sem)
    own_copy.start()
    lax.fori_loop(1, n, greet, 0)
    pl.semaphore_wait(barrier, n - 1)
    lax.fori_loop(1, n, send, 0)
    lax.fori_loop(1, n, finish, 0)
    own_copy.wait()


def exchange(vectors, n, number):
    length = vectors[0].shape[0]
    packed = jnp.concatenate(vectors).reshape(-1, 128)
    out = pl.pallas_call(
        functools.partial(exchange_kernel, n),
        out_shape=jax.ShapeDtypeStruct((n,) + packed.shape, jnp.float32),
        in_specs=[pl.BlockSpec(memory_space=pltpu.VMEM)],
        out_specs=pl.BlockSpec(memory_space=pltpu.VMEM),
        scratch_shapes=[
            pltpu.SemaphoreType.DMA,
            pltpu.SemaphoreType.DMA((n,)),
            pltpu.SemaphoreType.DMA((n,)),
        ],
        compiler_params=pltpu.CompilerParams(collective_id=number, has_side_effects=True),
        name="exchange",
    )(packed)
    return out.reshape(n, len(vectors), length // 128, 128)


def body(
    n, hidden, norm_gain, lm_head, draft_logits, draft_tokens, tree_parents, node_depths, uniforms
):
    vocab_dev = lm_head.shape[1]
    rows_all = draft_tokens.shape[0]
    requests = rows_all // NODES
    offset = lax.axis_index("vocab") * vocab_dev
    normed = normalize(hidden, norm_gain)
    local_column = draft_tokens - offset
    owned_here = (local_column >= 0) & (local_column < vocab_dev)
    vocab_iota = jnp.arange(vocab_dev, dtype=jnp.int32)
    column_hot = (local_column[:, None] == vocab_iota[None, :]) & owned_here[:, None]
    column_float = column_hot.astype(jnp.float32)
    column_half = column_hot.astype(jnp.bfloat16)
    node_iota = jnp.arange(NODES, dtype=jnp.int32)
    parent_hot = (
        tree_parents.reshape(requests, NODES)[:, :, None] == node_iota[None, None, :]
    ).astype(jnp.float32)

    def at_parent(vector):
        return jnp.einsum(
            "rkn,rn->rk", parent_hot, vector.reshape(requests, NODES), precision=highest
        ).reshape(rows_all)

    logits = gather_dot(normed, lm_head, n)
    draft_values = draft_logits.astype(jnp.float32)
    local_target = jnp.max(logits, axis=1)
    local_draft = jnp.max(draft_values, axis=1)
    stats = exchange(
        (
            local_target,
            jnp.sum(jnp.exp(logits - local_target[:, None]), axis=1),
            local_draft,
            jnp.sum(jnp.exp(draft_values - local_draft[:, None]), axis=1),
        ),
        n,
        1,
    )

    def joined(maxima, sums):
        top = jnp.max(maxima, axis=0)
        total = jnp.sum(sums * jnp.exp(maxima - top), axis=0)
        return (top + jnp.log(total)).reshape(rows_all)

    target_lse = joined(stats[:, 0], stats[:, 1])
    draft_lse = joined(stats[:, 2], stats[:, 3])
    excess = jnp.maximum(
        jnp.exp(logits - target_lse[:, None]) - jnp.exp(draft_values - draft_lse[:, None]), 0.0
    )
    target_cols = jnp.einsum(
        "rnv,rkv->rnk",
        logits.reshape(requests, NODES, vocab_dev),
        column_float.reshape(requests, NODES, vocab_dev),
        precision=highest,
    )
    draft_cols = jnp.einsum(
        "rnv,rkv->rnk",
        draft_logits.reshape(requests, NODES, vocab_dev),
        column_half.reshape(requests, NODES, vocab_dev),
        preferred_element_type=jnp.float32,
    )
    picked_target = jnp.sum(parent_hot * target_cols.transpose(0, 2, 1), axis=2).reshape(rows_all)
    picked_draft = jnp.sum(parent_hot * draft_cols.transpose(0, 2, 1), axis=2).reshape(rows_all)
    shares = exchange((jnp.sum(excess, axis=1), picked_target, picked_draft), n, 2)
    sums = jnp.sum(shares, axis=0).reshape(3, rows_all)
    residual_mass, picked_target, picked_draft = sums[0], sums[1], sums[2]
    token_logprob = picked_target - at_parent(target_lse)
    draft_logprob = picked_draft - at_parent(draft_lse)
    accept_margin = jnp.exp(jnp.minimum(token_logprob - draft_logprob, 0.0)) - uniforms
    path_margin = jnp.ones((rows_all,), jnp.float32)
    for level_now in range(1, DEPTH_MAX + 1):
        path_margin = jnp.where(
            node_depths == level_now,
            jnp.minimum(accept_margin, at_parent(path_margin)),
            path_margin,
        )
    return (target_lse, token_logprob, residual_mass, accept_margin, path_margin)


def solution(mesh):
    return jax.shard_map(
        functools.partial(body, mesh.shape["vocab"]),
        mesh=mesh,
        in_specs=(
            P(("batch", "vocab"), None),
            P(),
            P(None, "vocab"),
            P("batch", "vocab"),
            P("batch"),
            P("batch"),
            P("batch"),
            P("batch"),
        ),
        out_specs=(P("batch"), P("batch"), P("batch"), P("batch"), P("batch")),
        check_vma=False,
    )
```

```python
import functools

import jax
import jax.numpy as jnp
from jax import lax
from jax.experimental import pallas as pl
from jax.experimental.pallas import tpu as pltpu
from jax.sharding import PartitionSpec as P

NODES = 64
DEPTH_MAX = 8
MESH = pl.DeviceIdType.MESH
CHUNK_ROWS = 256
COLUMN_TILE = 256


epsilon = 1e-06
highest = lax.Precision.HIGHEST


def normalize(hidden_rows, gain_vector):
    values = hidden_rows.astype(jnp.float32)
    mean_square = jnp.mean(values * values, axis=1, keepdims=True)
    scaled = values * lax.rsqrt(mean_square + epsilon) * gain_vector.astype(jnp.float32)
    return scaled.astype(jnp.bfloat16)


CYCLES = (
    (0, 1, 3, 2, 6, 7, 5, 9, 11, 10, 14, 15, 13, 12, 8, 4),
    (0, 1, 5, 4, 6, 10, 8, 9, 13, 12, 14, 15, 11, 7, 3, 2),
    (0, 2, 6, 7, 3, 1, 5, 9, 13, 15, 11, 10, 14, 12, 8, 4),
)
LANE = 128


def look_up(table, index):
    value = jnp.int32(table[0])
    for k in range(1, len(table)):
        value = jnp.where(index == k, jnp.int32(table[k]), value)
    return value


def place_of(device, cycle, n):
    if n != 16:
        return device
    order = CYCLES[cycle]
    return look_up([order.index(k) for k in range(n)], device)


def device_at(place, cycle, n):
    if n != 16:
        return place
    return look_up(CYCLES[cycle], place)


def gather_dot_kernel(
    n, starts, widths, *refs
):
    streams = len(widths)
    owns, (head_ref, out_ref), helds = refs[:streams], refs[streams : streams + 2], refs[streams + 2 : -5]
    head, own_sem, head_sem, send_sem, recv_sem = refs[-5:]
    rows = owns[0].shape[0]
    group = max(1, min(n, CHUNK_ROWS // rows))
    chunks = n // group
    columns = out_ref.shape[2]
    me = lax.axis_index("vocab")
    places = [place_of(me, cycle, n) for cycle in range(3)]

    def stream_kind(q):
        return q // 2, q % 2

    def partner(q, steps):
        cycle, backward = stream_kind(q)
        hop = (n - steps) if backward else steps
        return device_at(lax.rem(places[cycle] + hop, n), cycle, n)

    own_copies = [
        pltpu.make_async_copy(owns[q], helds[q].at[0], own_sem.at[q]) for q in range(streams)
    ]
    for own_copy in own_copies:
        own_copy.start()
    head_copy = pltpu.make_async_copy(head_ref, head, head_sem)
    head_copy.start()

    ways = [partner(q, 1) for q in range(streams)]
    barrier = pltpu.get_barrier_semaphore()
    for target in ways:
        pl.semaphore_signal(barrier, inc=1, device_id={"vocab": target}, device_id_type=MESH)
    pl.semaphore_wait(barrier, len(ways))

    def copy_of(q, step):
        return pltpu.make_async_remote_copy(
            src_ref=helds[q].at[step],
            dst_ref=helds[q].at[step + 1],
            send_sem=send_sem.at[step, q],
            recv_sem=recv_sem.at[step, q],
            device_id={"vocab": ways[q]},
            device_id_type=MESH,
        )

    def multiply(chunk, q):
        first = chunk * group
        cycle, backward = stream_kind(q)
        owners = []
        for g in range(group):
            slot = first + g
            place = places[cycle] + slot if backward else places[cycle] + n - slot
            owners.append(device_at(lax.rem(place, n), cycle, n))

        def tile(index, _):
            at = pl.multiple_of(index * COLUMN_TILE, COLUMN_TILE)
            block = jnp.concatenate([helds[q][first + g] for g in range(group)], axis=0)
            part = jnp.dot(
                block, head[starts[q] : starts[q] + widths[q], pl.ds(at, COLUMN_TILE)], preferred_element_type=jnp.float32
            )
            for g in range(group):
                piece = part[g * rows : (g + 1) * rows]
                out_ref[owners[g], :, pl.ds(at, COLUMN_TILE)] += piece
            return 0

        lax.fori_loop(0, columns // COLUMN_TILE, tile, 0)

    for own_copy in own_copies:
        own_copy.wait()
    for q in range(streams):
        copy_of(q, 0).start()
    head_copy.wait()
    out_ref[...] = jnp.zeros_like(out_ref)

    return me, group, chunks, copy_of, multiply


def gather_dot_body(n, starts, widths, *refs):
    streams = len(widths)
    _, group, chunks, copy_of, multiply = gather_dot_kernel(n, starts, widths, *refs)
    per_step = -(-streams // group)
    spread = -(-streams // per_step)

    def run(chunk, turn):
        for k in range(per_step):
            q = turn * per_step + k
            if q < streams:
                multiply(chunk, q)

    def move(step):
        for q in range(streams):
            copy_of(q, step - 1).wait_recv()
            copy_of(q, step).start()

    def chunk_loop(chunk, _):
        for g in range(group):
            move(chunk * group + g)
            if g < spread:
                run(chunk - 1, g)
        return 0

    for step in range(1, group):
        move(step)
    lax.fori_loop(1, chunks - 1, chunk_loop, 0)
    for g in range(group):
        step = (chunks - 1) * group + g
        if step < n - 1:
            move(step)
        else:
            for q in range(streams):
                copy_of(q, step - 1).wait_recv()
        if g < spread:
            run(chunks - 2, g)
    for q in range(streams):
        multiply(chunks - 1, q)

    def drain(step, _):
        for q in range(streams):
            copy_of(q, step).wait_send()
        return 0

    lax.fori_loop(0, n - 1, drain, 0)


def gather_dot(normed, lm_head, n):
    rows, depth = normed.shape
    streams = 2 * len(CYCLES)
    tiles = depth // LANE
    pairs = [tiles // 2 * k // len(CYCLES) for k in range(len(CYCLES) + 1)]
    widths = [LANE * (pairs[q // 2 + 1] - pairs[q // 2]) for q in range(streams)]
    starts = [sum(widths[:q]) for q in range(streams)]
    columns = lm_head.shape[1]
    owns = [normed[:, at : at + width] for at, width in zip(starts, widths)]
    out = pl.pallas_call(
        functools.partial(gather_dot_body, n, starts, widths),
        out_shape=jax.ShapeDtypeStruct((n, rows, columns), jnp.float32),
        in_specs=[pl.BlockSpec(memory_space=pl.ANY)] * (streams + 1),
        out_specs=pl.BlockSpec(memory_space=pltpu.VMEM),
        scratch_shapes=[
            *(pltpu.VMEM((n, rows, width), jnp.bfloat16) for width in widths),
            pltpu.VMEM((depth, columns), jnp.bfloat16),
            pltpu.SemaphoreType.DMA((streams,)),
            pltpu.SemaphoreType.DMA,
            pltpu.SemaphoreType.DMA((n - 1, streams)),
            pltpu.SemaphoreType.DMA((n - 1, streams)),
        ],
        compiler_params=pltpu.CompilerParams(
            collective_id=0, has_side_effects=True, vmem_limit_bytes=56 * 1024 * 1024
        ),
        name="gather_dot",
    )(*owns, lm_head)
    return out.reshape(n * rows, columns)


def exchange_kernel(n, x_ref, out_ref, own_sem, send_sem, recv_sem):
    me = lax.axis_index("vocab")
    barrier = pltpu.get_barrier_semaphore()

    def copy_to(d):
        return pltpu.make_async_remote_copy(
            src_ref=x_ref,
            dst_ref=out_ref.at[me],
            send_sem=send_sem.at[d],
            recv_sem=recv_sem.at[d],
            device_id={"vocab": lax.rem(me + d, n)},
            device_id_type=MESH,
        )

    def copy_from(d):
        return pltpu.make_async_remote_copy(
            src_ref=x_ref,
            dst_ref=out_ref.at[lax.rem(me + n - d, n)],
            send_sem=send_sem.at[d],
            recv_sem=recv_sem.at[d],
            device_id={"vocab": lax.rem(me + d, n)},
            device_id_type=MESH,
        )

    def greet(d, _):
        pl.semaphore_signal(
            barrier, inc=1, device_id={"vocab": lax.rem(me + d, n)}, device_id_type=MESH
        )
        return 0

    def send(d, _):
        copy_to(d).start()
        return 0

    def finish(d, _):
        copy_from(d).wait_recv()
        copy_to(d).wait_send()
        return 0

    own_copy = pltpu.make_async_copy(x_ref, out_ref.at[me], own_sem)
    own_copy.start()
    lax.fori_loop(1, n, greet, 0)
    pl.semaphore_wait(barrier, n - 1)
    lax.fori_loop(1, n, send, 0)
    lax.fori_loop(1, n, finish, 0)
    own_copy.wait()


def exchange(vectors, n, number):
    length = vectors[0].shape[0]
    packed = jnp.concatenate(vectors).reshape(-1, 128)
    out = pl.pallas_call(
        functools.partial(exchange_kernel, n),
        out_shape=jax.ShapeDtypeStruct((n,) + packed.shape, jnp.float32),
        in_specs=[pl.BlockSpec(memory_space=pltpu.VMEM)],
        out_specs=pl.BlockSpec(memory_space=pltpu.VMEM),
        scratch_shapes=[
            pltpu.SemaphoreType.DMA,
            pltpu.SemaphoreType.DMA((n,)),
            pltpu.SemaphoreType.DMA((n,)),
        ],
        compiler_params=pltpu.CompilerParams(collective_id=number, has_side_effects=True),
        name="exchange",
    )(packed)
    return out.reshape(n, len(vectors), length // 128, 128)


def body(
    n, hidden, norm_gain, lm_head, draft_logits, draft_tokens, tree_parents, node_depths, uniforms
):
    vocab_dev = lm_head.shape[1]
    rows_all = draft_tokens.shape[0]
    requests = rows_all // NODES
    offset = lax.axis_index("vocab") * vocab_dev
    normed = normalize(hidden, norm_gain)
    local_column = draft_tokens - offset
    owned_here = (local_column >= 0) & (local_column < vocab_dev)
    vocab_iota = jnp.arange(vocab_dev, dtype=jnp.int32)
    column_hot = (local_column[:, None] == vocab_iota[None, :]) & owned_here[:, None]
    column_float = column_hot.astype(jnp.float32)
    column_half = column_hot.astype(jnp.bfloat16)
    node_iota = jnp.arange(NODES, dtype=jnp.int32)
    parent_hot = (
        tree_parents.reshape(requests, NODES)[:, :, None] == node_iota[None, None, :]
    ).astype(jnp.float32)

    def at_parent(vector):
        return jnp.einsum(
            "rkn,rn->rk", parent_hot, vector.reshape(requests, NODES), precision=highest
        ).reshape(rows_all)

    logits = gather_dot(normed, lm_head, n)
    draft_values = draft_logits.astype(jnp.float32)
    local_target = jnp.max(logits, axis=1)
    local_draft = jnp.max(draft_values, axis=1)
    stats = exchange(
        (
            local_target,
            jnp.sum(jnp.exp(logits - local_target[:, None]), axis=1),
            local_draft,
            jnp.sum(jnp.exp(draft_values - local_draft[:, None]), axis=1),
        ),
        n,
        1,
    )

    def joined(maxima, sums):
        top = jnp.max(maxima, axis=0)
        total = jnp.sum(sums * jnp.exp(maxima - top), axis=0)
        return (top + jnp.log(total)).reshape(rows_all)

    target_lse = joined(stats[:, 0], stats[:, 1])
    draft_lse = joined(stats[:, 2], stats[:, 3])
    excess = jnp.maximum(
        jnp.exp(logits - target_lse[:, None]) - jnp.exp(draft_values - draft_lse[:, None]), 0.0
    )
    target_cols = jnp.einsum(
        "rnv,rkv->rnk",
        logits.reshape(requests, NODES, vocab_dev),
        column_float.reshape(requests, NODES, vocab_dev),
        precision=highest,
    )
    draft_cols = jnp.einsum(
        "rnv,rkv->rnk",
        draft_logits.reshape(requests, NODES, vocab_dev),
        column_half.reshape(requests, NODES, vocab_dev),
        preferred_element_type=jnp.float32,
    )
    picked_target = jnp.sum(parent_hot * target_cols.transpose(0, 2, 1), axis=2).reshape(rows_all)
    picked_draft = jnp.sum(parent_hot * draft_cols.transpose(0, 2, 1), axis=2).reshape(rows_all)
    shares = exchange((jnp.sum(excess, axis=1), picked_target, picked_draft), n, 2)
    sums = jnp.sum(shares, axis=0).reshape(3, rows_all)
    residual_mass, picked_target, picked_draft = sums[0], sums[1], sums[2]
    token_logprob = picked_target - at_parent(target_lse)
    draft_logprob = picked_draft - at_parent(draft_lse)
    accept_margin = jnp.exp(jnp.minimum(token_logprob - draft_logprob, 0.0)) - uniforms
    path_margin = jnp.ones((rows_all,), jnp.float32)
    for level_now in range(1, DEPTH_MAX + 1):
        path_margin = jnp.where(
            node_depths == level_now,
            jnp.minimum(accept_margin, at_parent(path_margin)),
            path_margin,
        )
    return (target_lse, token_logprob, residual_mass, accept_margin, path_margin)


def solution(mesh):
    return jax.shard_map(
        functools.partial(body, mesh.shape["vocab"]),
        mesh=mesh,
        in_specs=(
            P(("batch", "vocab"), None),
            P(),
            P(None, "vocab"),
            P("batch", "vocab"),
            P("batch"),
            P("batch"),
            P("batch"),
            P("batch"),
        ),
        out_specs=(P("batch"), P("batch"), P("batch"), P("batch"), P("batch")),
        check_vma=False,
    )
```
